8 devices in a mesh: part: 1 (over z), row: 2 (over y), col: 4 (over x, core).
Axes of the slice: x: 2, y: 2, z: 1, core: 2. Of those that a mesh axis runs over, the one named last changes fastest.
Arguments:
- counts: bfloat16 [4096, 32768], P(('part', 'row'), 'col')
- w_init: float32 [4096, 1024], P(('part', 'row'))
- h_init: float32 [1024, 32768], P('part', 'col')
Outputs:
- output 1: float32 [4096, 1024], P(('part', 'row'))
- output 2: float32 [1024, 32768], P('part', 'col')
All inputs are finite; a program needn't handle non-finite values.
Results may differ from the reference program's by a relative error of at most 0.001.
Values are sent between devices in bfloat16 or wider.
A program may use at most 1 GiB of HBM per device.

```python
import jax
import jax.numpy as jnp
from jax import lax

DOCS = 4096
VOCAB = 32768
TOPICS = 1024
SWEEPS = 6
BLOCK_ROWS = 256


def setup_inputs(seed: int = 0, part: int = 0) -> dict:
    root_key = jax.random.fold_in(jax.random.key(seed), part)
    key_row, key_col, key_cnt, key_w, key_h = jax.random.split(root_key, 5)
    row_level = jax.random.randint(key_row, (DOCS, 1), 1, 5)
    col_level = jax.random.randint(key_col, (1, VOCAB), 1, 5)
    raw_bits = jax.random.randint(key_cnt, (DOCS, VOCAB), 0, 2 ** 20)
    counts = raw_bits % (1 + row_level * col_level)
    init_scale = (3.0 / TOPICS) ** 0.5
    w_init = jax.random.uniform(key_w, (DOCS, TOPICS), jnp.float32, 0.25, 1.75) * init_scale
    h_init = jax.random.uniform(key_h, (TOPICS, VOCAB), jnp.float32, 0.25, 1.75) * init_scale
    return {"counts": counts.astype(jnp.float32).astype(jnp.bfloat16), "w_init": w_init, "h_init": h_init}


def reference(counts, w_init, h_init):
    num_blocks = DOCS // BLOCK_ROWS
    count_blocks = counts.reshape(num_blocks, BLOCK_ROWS, VOCAB)

    def one_sweep(carry_state, sweep_idx):
        w_state, h_state = carry_state
        w_bf = w_state.astype(jnp.bfloat16)
        h_bf = h_state.astype(jnp.bfloat16)
        h_rowsum = jnp.sum(h_state, axis=1)
        w_colsum = jnp.sum(w_state, axis=0)

        def one_block(acc_h, block_in):
            count_blk, w_blk = block_in
            z_blk = jnp.dot(w_blk, h_bf, preferred_element_type=jnp.float32)
            q_blk = (count_blk.astype(jnp.float32) / z_blk).astype(jnp.bfloat16)
            num_w = jnp.dot(q_blk, h_bf.T, preferred_element_type=jnp.float32)
            acc_h = acc_h + jnp.dot(w_blk.T, q_blk, preferred_element_type=jnp.float32)
            return acc_h, num_w

        num_h, num_w = lax.scan(one_block, jnp.zeros((TOPICS, VOCAB), jnp.float32), (count_blocks, w_bf.reshape(num_blocks, BLOCK_ROWS, TOPICS)))
        w_next = w_state * num_w.reshape(DOCS, TOPICS) / h_rowsum[None, :]
        h_next = h_state * num_h / w_colsum[:, None]
        return (w_next, h_next), None

    final_state, unused = lax.scan(one_sweep, (w_init, h_init), None, length=SWEEPS)
    return final_state[0], final_state[1]
```

```python
import functools

import jax
import jax.numpy as jnp
from jax import lax
from jax.experimental import pallas as pl
from jax.experimental.pallas import tpu as pltpu
from jax.sharding import PartitionSpec as P


SWEEPS = 6
BLK = 256
COLBLK = 1024
AXES = ("row", "col")
F32 = jnp.float32
BF16 = jnp.bfloat16


def swap(val, mask):
    return lax.ppermute(val, AXES, [(i, i ^ mask) for i in range(8)])


def swap_by_core(val, mask0, mask1):
    return lax.ppermute(val, AXES, [(i, i ^ (mask1 if i & 1 else mask0)) for i in range(8)])


def dot_nw(q, h_bf):
    return lax.dot_general(q, h_bf, (((1,), (1,)), ((), ())), preferred_element_type=F32)


def dot_nh(w_bf, q):
    return lax.dot_general(w_bf, q, (((0,), (0,)), ((), ())), preferred_element_type=F32)


def quotient(counts, w_bf, h_bf):
    return (counts.astype(F32) / jnp.dot(w_bf, h_bf, preferred_element_type=F32)).astype(BF16)


def pick(arr, idx, axis):
    return lax.dynamic_index_in_dim(arr, idx, axis, keepdims=False)


def assemble_kernel(keys, axis_col, *refs):
    pieces, out_ref, sems = refs[:len(keys)], refs[-2], refs[-1]
    col = lax.axis_index(axis_col)
    core, chip = lax.rem(col, 2), lax.div(col, 2)
    copies = []
    for n, (yrel, xrel, crel) in enumerate(keys):
        core_at = 1 - core if crel else core
        chip_at = 1 - chip if xrel else chip
        start = pl.multiple_of(yrel * 1024 + core_at * 512 + chip_at * BLK, BLK)
        copy = pltpu.make_async_copy(pieces[n], out_ref.at[pl.ds(start, BLK)], sems.at[n])
        copy.start()
        copies.append(copy)
    for copy in copies:
        copy.wait()


def assemble(pieces):
    keys = tuple(pieces)
    val = next(iter(pieces.values()))
    size = len(keys) * BLK
    return pl.pallas_call(
        functools.partial(assemble_kernel, keys, "col"),
        out_shape=jax.ShapeDtypeStruct((size, val.shape[1]), val.dtype),
        in_specs=[pl.BlockSpec(memory_space=pl.ANY)] * len(keys),
        out_specs=pl.BlockSpec(memory_space=pltpu.VMEM),
        scratch_shapes=[pltpu.SemaphoreType.DMA((len(keys),))],
        cost_estimate=pl.CostEstimate(flops=10 ** 9, bytes_accessed=4 * size * val.shape[1], transcendentals=0),
    )(*[pieces[k] for k in keys])


def join_kernel(side_ref, own_ref, oth_ref, out_ref):
    step = pl.program_id(0)

    @pl.when(step < 4)
    def _():
        out_ref[...] = own_ref[...]

    @pl.when(step >= 4)
    def _():
        out_ref[...] = oth_ref[...]


def join_rows(side, c_blk, first_row, c_oth):
    width = c_oth.shape[1]
    base = first_row // BLK
    return pl.pallas_call(
        join_kernel,
        out_shape=jax.ShapeDtypeStruct((2048, width), BF16),
        grid_spec=pltpu.PrefetchScalarGridSpec(
            num_scalar_prefetch=1,
            grid=(8,),
            in_specs=[
                pl.BlockSpec((BLK, width), lambda i, s: (base + jnp.minimum(i, 3), s[0])),
                pl.BlockSpec((BLK, width), lambda i, s: (jnp.maximum(i - 4, 0), 0)),
            ],
            out_specs=pl.BlockSpec((BLK, width), lambda i, s: (i, 0)),
        ),
        cost_estimate=pl.CostEstimate(flops=10 ** 9, bytes_accessed=4 * 2048 * width, transcendentals=0),
    )(jnp.reshape(side, (1,)).astype(jnp.int32), c_blk, c_oth)


def butterfly(vec):
    for mask in (1, 2, 4):
        vec = vec + swap(vec, mask)
    return vec


def solution(mesh):
    def body(c_blk, w_blk, h_blk):
        side = lax.axis_index("row")
        col = lax.axis_index("col")
        core, chip = lax.rem(col, 2), lax.div(col, 2)
        half = h_blk.shape[1] // 2
        mine = side * half
        theirs = (1 - side) * half

        def reduce_set_x(num):
            view = num.reshape(2, 2, 2, BLK, 1024)
            tot = pick(view, core, 1) + swap(pick(view, 1 - core, 1), 1)
            tot = pick(tot, chip, 1) + swap(pick(tot, 1 - chip, 1), 2)
            return tot[0] + swap(tot[1], 4)

        def reduce_set(num):
            view = num.reshape(2, 2, 2, BLK, 1024)
            got = swap(pick(view, 1 - core, 1), 1)
            tot = pick(view, core, 1) + got
            send = jnp.where(core == 0, pick(tot, 1 - chip, 1), tot[1])
            keep = jnp.where(core == 0, pick(tot, chip, 1), tot[0])
            keep = keep + swap_by_core(send, 2, 4)
            away = jnp.where(core == 0, 1, 1 - chip)
            got = swap_by_core(pick(keep, away, 0), 4, 2)
            return pick(keep, 1 - away, 0) + got

        def gather_set(b0):
            pieces = {(0, 0, 0): b0}
            for y, x in ((0, 1), (1, 0), (1, 1)):
                pieces[(y, x, 0)] = swap(b0, 4 * y + 2 * x)
            for y, x in ((0, 0), (0, 1), (1, 0), (1, 1)):
                pieces[(y, x, 1)] = swap(pieces[(y, x, 0)], 1)
            return assemble(pieces)

        def sums(h_part, w_val):
            part = jnp.stack([h_part, jnp.sum(w_val[0], axis=0) + jnp.sum(w_val[1], axis=0)])
            tot = butterfly(part)
            return tot[0], tot[1]

        c_oth = []
        for s in range(2):
            sent = lax.dynamic_slice(c_blk, (s * 1024, theirs), (1024, half))
            c_oth.append(swap(sent, 4))
        h_state = lax.dynamic_slice_in_dim(h_blk, mine, half, 1)
        hb = h_state.astype(BF16)
        hb_theirs = lax.dynamic_slice_in_dim(h_blk, theirs, half, 1).astype(BF16)
        w_own = w_blk.astype(BF16)
        offset = core * 512 + chip * BLK
        w_state = [lax.dynamic_slice_in_dim(w_blk, s * 1024 + offset, BLK, 0) for s in range(2)]
        w_oth = []
        for s in range(2):
            b0 = w_state[s].astype(BF16)
            p10 = swap(b0, 4)
            p11 = swap(b0, 6)
            pieces = {(0, 0, 0): p10, (0, 1, 0): p11, (0, 0, 1): swap(p10, 1), (0, 1, 1): swap(p11, 1)}
            w_oth.append(assemble(pieces))
        h_sum, w_sum = sums(jnp.sum(h_state, axis=1), w_state)
        q_theirs = quotient(lax.dynamic_slice_in_dim(c_blk, theirs, half, 1), w_own, hb_theirs)
        num_t = dot_nw(q_theirs, hb_theirs)
        q_own = quotient(lax.dynamic_slice_in_dim(c_blk, mine, half, 1), w_own, hb)
        num_w = num_t + dot_nw(q_own, hb)
        view = num_w.reshape(2, 2, 2, BLK, 1024)
        tot = pick(view, core, 1) + swap(pick(view, 1 - core, 1), 1)
        num_w = pick(tot, chip, 1) + swap(pick(tot, 1 - chip, 1), 2)
        num_h = dot_nh(w_own, q_own)
        w_state = [lax.optimization_barrier(w_state[s] * num_w[s] / h_sum[None, :]) for s in range(2)]
        w_set = [gather_set(w_state[s].astype(BF16)) for s in range(2)]
        for s in range(2):
            q_oth = quotient(c_oth[s], w_oth[s], hb)
            num_h = num_h + dot_nh(w_oth[s], q_oth)
        counts = [join_rows(side, c_blk, s * 1024, c_oth[s]) for s in range(2)]
        h_state = h_state * num_h / w_sum[:, None]
        hb = h_state.astype(BF16)
        h_part = jnp.sum(h_state, axis=1)

        for _ in range(1, SWEEPS - 1):
            h_sum, w_sum = sums(h_part, w_state)
            q_set, w_next, w_gathered = [], [], []
            for s in range(2):
                q_set.append(quotient(counts[s], w_set[s], hb))
                num_w = reduce_set(dot_nw(q_set[s], hb))
                num_w, h_tot = lax.optimization_barrier((num_w, h_sum))
                w_next.append(lax.optimization_barrier(w_state[s] * num_w / h_tot[None, :]))
                w_gathered.append(gather_set(w_next[s].astype(BF16)))
            num_h = dot_nh(w_set[0], q_set[0]) + dot_nh(w_set[1], q_set[1])
            h_state = h_state * num_h / w_sum[:, None]
            hb = h_state.astype(BF16)
            h_part = jnp.sum(h_state, axis=1)
            w_state = w_next
            w_set = w_gathered

        h_sum, w_sum = sums(h_part, w_state)
        h_out = jnp.zeros(h_blk.shape, F32)
        num_w = [None, None]
        for j in range(half // COLBLK):
            at = slice(j * COLBLK, (j + 1) * COLBLK)
            q_set = [quotient(counts[s][:, at], w_set[s], hb[:, at]) for s in range(2)]
            num_h = dot_nh(w_set[0], q_set[0]) + dot_nh(w_set[1], q_set[1])
            h_fin = h_state[:, at] * num_h / w_sum[:, None]
            h_got = swap(h_fin, 4)
            h_out = lax.dynamic_update_slice_in_dim(h_out, h_fin, mine + j * COLBLK, 1)
            h_out = lax.dynamic_update_slice_in_dim(h_out, h_got, theirs + j * COLBLK, 1)
            for s in range(2):
                part = dot_nw(q_set[s], hb[:, at])
                num_w[s] = part if num_w[s] is None else num_w[s] + part
        w_out = jnp.zeros(w_blk.shape, F32)
        w_fin = []
        for s in range(2):
            tot = reduce_set_x(num_w[s])
            w_fin.append(w_state[s] * tot / h_sum[None, :])
        w_fin = jnp.stack(w_fin)
        w_x = swap(w_fin, 2)
        got = [(0, 0, w_fin), (1, 0, w_x), (0, 1, swap(w_fin, 1)), (1, 1, swap(w_x, 1))]
        for x, c, val in got:
            start = jnp.bitwise_xor(core, c) * 512 + jnp.bitwise_xor(chip, x) * BLK
            for s in range(2):
                w_out = lax.dynamic_update_slice_in_dim(w_out, val[s], s * 1024 + start, 0)
        return w_out, h_out


    return jax.shard_map(
        body,
        mesh=mesh,
        in_specs=(P(("part", "row"), "col"), P(("part", "row"), None), P("part", "col")),
        out_specs=(P(("part", "row"), None), P("part", "col")),
        check_vma=False,
    )
```

```python
import functools

import jax
import jax.numpy as jnp
from jax import lax
from jax.experimental import pallas as pl
from jax.experimental.pallas import tpu as pltpu
from jax.sharding import PartitionSpec as P


SWEEPS = 6
BLK = 256
CUTS = (0, 512, 1536, 2560, 3584, 4096)
AXES = ("row", "col")
F32 = jnp.float32
BF16 = jnp.bfloat16


def swap(val, mask):
    return lax.ppermute(val, AXES, [(i, i ^ mask) for i in range(8)])


def swap_by_core(val, mask0, mask1):
    return lax.ppermute(val, AXES, [(i, i ^ (mask1 if i & 1 else mask0)) for i in range(8)])


def dot_nw(q, h_bf):
    return lax.dot_general(q, h_bf, (((1,), (1,)), ((), ())), preferred_element_type=F32)


def dot_nh(w_bf, q):
    return lax.dot_general(w_bf, q, (((0,), (0,)), ((), ())), preferred_element_type=F32)


def quotient(counts, w_bf, h_bf):
    return (counts.astype(F32) / jnp.dot(w_bf, h_bf, preferred_element_type=F32)).astype(BF16)


def pick(arr, idx, axis):
    return lax.dynamic_index_in_dim(arr, idx, axis, keepdims=False)


def assemble_kernel(keys, axis_col, *refs):
    pieces, out_ref, sems = refs[:len(keys)], refs[-2], refs[-1]
    col = lax.axis_index(axis_col)
    core, chip = lax.rem(col, 2), lax.div(col, 2)
    copies = []
    for n, (yrel, xrel, crel) in enumerate(keys):
        core_at = 1 - core if crel else core
        chip_at = 1 - chip if xrel else chip
        start = pl.multiple_of(yrel * 1024 + core_at * 512 + chip_at * BLK, BLK)
        copy = pltpu.make_async_copy(pieces[n], out_ref.at[pl.ds(start, BLK)], sems.at[n])
        copy.start()
        copies.append(copy)
    for copy in copies:
        copy.wait()


def assemble(pieces):
    keys = tuple(pieces)
    val = next(iter(pieces.values()))
    size = len(keys) * BLK
    return pl.pallas_call(
        functools.partial(assemble_kernel, keys, "col"),
        out_shape=jax.ShapeDtypeStruct((size, val.shape[1]), val.dtype),
        in_specs=[pl.BlockSpec(memory_space=pl.ANY)] * len(keys),
        out_specs=pl.BlockSpec(memory_space=pltpu.VMEM),
        scratch_shapes=[pltpu.SemaphoreType.DMA((len(keys),))],
        cost_estimate=pl.CostEstimate(flops=10 ** 9, bytes_accessed=4 * size * val.shape[1], transcendentals=0),
    )(*[pieces[k] for k in keys])


def join_kernel(side_ref, own_ref, oth0_ref, oth1_ref, out_ref):
    step = pl.program_id(0)

    @pl.when(step < 4)
    def _():
        out_ref[...] = own_ref[...]

    @pl.when((step >= 4) & (step < 6))
    def _():
        out_ref[...] = oth0_ref[...]

    @pl.when(step >= 6)
    def _():
        out_ref[...] = oth1_ref[...]


def join_rows(side, c_blk, first_row, c_oth):
    width = c_oth[0].shape[1]
    base = first_row // BLK
    return pl.pallas_call(
        join_kernel,
        out_shape=jax.ShapeDtypeStruct((2048, width), BF16),
        grid_spec=pltpu.PrefetchScalarGridSpec(
            num_scalar_prefetch=1,
            grid=(8,),
            in_specs=[
                pl.BlockSpec((BLK, width), lambda i, s: (base + jnp.minimum(i, 3), s[0])),
                pl.BlockSpec((BLK, width), lambda i, s: (jnp.clip(i - 4, 0, 1), 0)),
                pl.BlockSpec((BLK, width), lambda i, s: (jnp.clip(i - 6, 0, 1), 0)),
            ],
            out_specs=pl.BlockSpec((BLK, width), lambda i, s: (i, 0)),
        ),
        cost_estimate=pl.CostEstimate(flops=10 ** 9, bytes_accessed=4 * 2048 * width, transcendentals=0),
    )(jnp.reshape(side, (1,)).astype(jnp.int32), c_blk, *c_oth)


def butterfly(vec):
    for mask in (1, 2, 4):
        vec = vec + swap(vec, mask)
    return vec


def solution(mesh):
    def body(c_blk, w_blk, h_blk):
        side = lax.axis_index("row")
        col = lax.axis_index("col")
        core, chip = lax.rem(col, 2), lax.div(col, 2)
        half = h_blk.shape[1] // 2
        mine = side * half
        theirs = (1 - side) * half

        def reduce_set_x(num):
            view = num.reshape(2, 2, 2, BLK, 1024)
            tot = pick(view, core, 1) + swap(pick(view, 1 - core, 1), 1)
            tot = pick(tot, chip, 1) + swap(pick(tot, 1 - chip, 1), 2)
            return tot[0] + swap(tot[1], 4)

        def reduce_set(num):
            view = num.reshape(2, 2, 2, BLK, 1024)
            got = swap(pick(view, 1 - core, 1), 1)
            tot = pick(view, core, 1) + got
            send = jnp.where(core == 0, pick(tot, 1 - chip, 1), tot[1])
            keep = jnp.where(core == 0, pick(tot, chip, 1), tot[0])
            keep = keep + swap_by_core(send, 2, 4)
            away = jnp.where(core == 0, 1, 1 - chip)
            got = swap_by_core(pick(keep, away, 0), 4, 2)
            return pick(keep, 1 - away, 0) + got

        def gather_set(b0, relay=False):
            pieces = {(0, 0, 0): b0}
            for y, x in ((0, 1), (1, 0), (1, 1)):
                if relay and y and x:
                    pieces[(y, x, 0)] = swap(pieces[(1, 0, 0)], 2)
                else:
                    pieces[(y, x, 0)] = swap(b0, 4 * y + 2 * x)
            for y, x in ((0, 0), (0, 1), (1, 0), (1, 1)):
                pieces[(y, x, 1)] = swap(pieces[(y, x, 0)], 1)
            return assemble(pieces)

        def sums(h_part, w_val):
            w_val = lax.optimization_barrier(tuple(w_val))
            part = jnp.stack([h_part, jnp.sum(w_val[0], axis=0) + jnp.sum(w_val[1], axis=0)])
            tot = butterfly(part)
            return tot[0], tot[1]

        c_oth = []
        for p in range(4):
            sent = lax.dynamic_slice(c_blk, (p * 512, theirs), (512, half))
            c_oth.append(swap(lax.optimization_barrier(sent), 4))
        h_state = lax.dynamic_slice_in_dim(h_blk, mine, half, 1)
        hb = h_state.astype(BF16)
        hb_theirs = lax.dynamic_slice_in_dim(h_blk, theirs, half, 1).astype(BF16)
        w_own = w_blk.astype(BF16)
        offset = core * 512 + chip * BLK
        w_state = [lax.dynamic_slice_in_dim(w_blk, s * 1024 + offset, BLK, 0) for s in range(2)]
        w_oth = []
        for s in range(2):
            b0 = w_state[s].astype(BF16)
            p10 = swap(b0, 4)
            p11 = swap(p10, 2)
            pieces = {(0, 0, 0): p10, (0, 1, 0): p11, (0, 0, 1): swap(p10, 1), (0, 1, 1): swap(p11, 1)}
            w_oth.append(assemble(pieces))
        w_sum = jnp.sum(w_blk, axis=0)[None, :]
        w_sum = (w_sum + swap(w_sum, 4))[0]
        h_sum = jnp.sum(h_blk, axis=1)[None, :]
        for mask in (1, 2):
            h_sum = h_sum + swap(h_sum, mask)
        h_sum = h_sum[0]
        q_theirs = quotient(lax.dynamic_slice_in_dim(c_blk, theirs, half, 1), w_own, hb_theirs)
        num_t = dot_nw(q_theirs, hb_theirs)
        q_own = quotient(lax.dynamic_slice_in_dim(c_blk, mine, half, 1), w_own, hb)
        num_w = num_t + dot_nw(q_own, hb)
        view = num_w.reshape(2, 2, 2, BLK, 1024)
        tot = pick(view, core, 1) + swap(pick(view, 1 - core, 1), 1)
        num_w = pick(tot, chip, 1) + swap(pick(tot, 1 - chip, 1), 2)
        num_h = dot_nh(w_own, q_own)
        w_state = [lax.optimization_barrier(w_state[s] * num_w[s] / h_sum[None, :]) for s in range(2)]
        w_set = [gather_set(w_state[s].astype(BF16), relay=True) for s in range(2)]
        for p in range(4):
            w_part = w_oth[p // 2][(p % 2) * 512:(p % 2) * 512 + 512]
            q_oth = quotient(c_oth[p], w_part, hb)
            num_h = num_h + dot_nh(w_part, q_oth)
        counts = [join_rows(side, c_blk, s * 1024, c_oth[2 * s:2 * s + 2]) for s in range(2)]
        h_state = h_state * num_h / w_sum[:, None]
        hb = h_state.astype(BF16)
        h_part = jnp.sum(h_state, axis=1)

        for _ in range(1, SWEEPS - 1):
            h_sum, w_sum = sums(h_part, w_state)
            q_set, w_next, w_gathered = [], [], []
            for s in range(2):
                q_set.append(quotient(counts[s], w_set[s], hb))
                num_w = reduce_set(dot_nw(q_set[s], hb))
                num_w, h_tot = lax.optimization_barrier((num_w, h_sum))
                w_next.append(lax.optimization_barrier(w_state[s] * num_w / h_tot[None, :]))
                w_gathered.append(gather_set(w_next[s].astype(BF16)))
            num_h = dot_nh(w_set[0], q_set[0]) + dot_nh(w_set[1], q_set[1])
            h_state = h_state * num_h / w_sum[:, None]
            hb = h_state.astype(BF16)
            h_part = jnp.sum(h_state, axis=1)
            w_state = w_next
            w_set = w_gathered

        h_sum, w_sum = sums(h_part, w_state)
        h_out = jnp.zeros(h_blk.shape, F32)
        num_w = [None, None]
        for lo, hi in zip(CUTS[:-1], CUTS[1:]):
            at = slice(lo, hi)
            q_set = [quotient(counts[s][:, at], w_set[s], hb[:, at]) for s in range(2)]
            num_h = dot_nh(w_set[0], q_set[0]) + dot_nh(w_set[1], q_set[1])
            h_fin = h_state[:, at] * num_h / w_sum[:, None]
            h_got = swap(h_fin, 4)
            h_out = lax.dynamic_update_slice_in_dim(h_out, h_fin, mine + lo, 1)
            if hi < half:
                h_out = lax.dynamic_update_slice_in_dim(h_out, h_got, theirs + lo, 1)
            for s in range(2):
                part = dot_nw(q_set[s], hb[:, at])
                num_w[s] = part if num_w[s] is None else num_w[s] + part
        w_out = jnp.zeros(w_blk.shape, F32)
        w_fin = []
        for s in range(2):
            tot = reduce_set_x(num_w[s])
            w_fin.append(w_state[s] * tot / h_sum[None, :])
        w_fin = jnp.stack(w_fin)
        w_x = swap(w_fin, 2)
        got = [(0, 0, w_fin), (1, 0, w_x), (0, 1, swap(w_fin, 1)), (1, 1, swap(w_x, 1))]
        for x, c, val in got:
            start = jnp.bitwise_xor(core, c) * 512 + jnp.bitwise_xor(chip, x) * BLK
            for s in range(2):
                w_out = lax.dynamic_update_slice_in_dim(w_out, val[s], s * 1024 + start, 0)
        w_out, h_got = lax.optimization_barrier((w_out, h_got))
        return w_out, lax.dynamic_update_slice_in_dim(h_out, h_got, theirs + CUTS[-2], 1)


    return jax.shard_map(
        body,
        mesh=mesh,
        in_specs=(P(("part", "row"), "col"), P(("part", "row"), None), P("part", "col")),
        out_specs=(P(("part", "row"), None), P("part", "col")),
        check_vma=False,
    )
```

```python
import functools

import jax
import jax.numpy as jnp
from jax import lax
from jax.experimental import pallas as pl
from jax.experimental.pallas import tpu as pltpu
from jax.experimental.layout import Layout, with_layout_constraint
from jax.sharding import PartitionSpec as P


SWEEPS = 6
BLK = 256
CUTS = (0, 512, 1536, 2560, 3584, 4096)
AXES = ("row", "col")
F32 = jnp.float32
BF16 = jnp.bfloat16


def swap(val, mask):
    return lax.ppermute(val, AXES, [(i, i ^ mask) for i in range(8)])


def swap_by_core(val, mask0, mask1):
    return lax.ppermute(val, AXES, [(i, i ^ (mask1 if i & 1 else mask0)) for i in range(8)])


def dot_nw(q, h_bf):
    return lax.dot_general(q, h_bf, (((1,), (1,)), ((), ())), preferred_element_type=F32)


def dot_nh(w_bf, q):
    return lax.dot_general(w_bf, q, (((0,), (0,)), ((), ())), preferred_element_type=F32)


def quotient(counts, w_bf, h_bf):
    return (counts.astype(F32) / jnp.dot(w_bf, h_bf, preferred_element_type=F32)).astype(BF16)


def pick(arr, idx, axis):
    return lax.dynamic_index_in_dim(arr, idx, axis, keepdims=False)


def assemble_kernel(keys, axis_col, *refs):
    pieces, out_ref, sems = refs[:len(keys)], refs[-2], refs[-1]
    col = lax.axis_index(axis_col)
    core, chip = lax.rem(col, 2), lax.div(col, 2)
    copies = []
    for n, (yrel, xrel, crel) in enumerate(keys):
        core_at = 1 - core if crel else core
        chip_at = 1 - chip if xrel else chip
        start = pl.multiple_of(yrel * 1024 + core_at * 512 + chip_at * BLK, BLK)
        copy = pltpu.make_async_copy(pieces[n], out_ref.at[pl.ds(start, BLK)], sems.at[n])
        copy.start()
        copies.append(copy)
    for copy in copies:
        copy.wait()


def assemble(pieces):
    keys = tuple(pieces)
    val = next(iter(pieces.values()))
    size = len(keys) * BLK
    return pl.pallas_call(
        functools.partial(assemble_kernel, keys, "col"),
        out_shape=jax.ShapeDtypeStruct((size, val.shape[1]), val.dtype),
        in_specs=[pl.BlockSpec(memory_space=pl.ANY)] * len(keys),
        out_specs=pl.BlockSpec(memory_space=pltpu.VMEM),
        scratch_shapes=[pltpu.SemaphoreType.DMA((len(keys),))],
        cost_estimate=pl.CostEstimate(flops=10 ** 9, bytes_accessed=4 * size * val.shape[1], transcendentals=0),
    )(*[pieces[k] for k in keys])


def join_kernel(side_ref, own_ref, oth_ref, out_ref):
    step = pl.program_id(0)

    @pl.when(step < 4)
    def _():
        out_ref[...] = own_ref[...]

    @pl.when(step >= 4)
    def _():
        out_ref[...] = oth_ref[...]


def append_kernel(all_ref, oth_ref, out_ref):
    out_ref[...] = oth_ref[...]


def join_rows(side, c_blk, first_row, c_oth):
    width = c_oth[0].shape[1]
    base = first_row // BLK
    out_shape = jax.ShapeDtypeStruct((2048, width), BF16)
    cost = pl.CostEstimate(flops=10 ** 9, bytes_accessed=4 * 1024 * width, transcendentals=0)
    most = pl.pallas_call(
        join_kernel,
        out_shape=out_shape,
        grid_spec=pltpu.PrefetchScalarGridSpec(
            num_scalar_prefetch=1,
            grid=(6,),
            in_specs=[
                pl.BlockSpec((BLK, width), lambda i, s: (base + jnp.minimum(i, 3), s[0])),
                pl.BlockSpec((BLK, width), lambda i, s: (jnp.maximum(i - 4, 0), 0)),
            ],
            out_specs=pl.BlockSpec((BLK, width), lambda i, s: (i, 0)),
        ),
        cost_estimate=cost,
    )(jnp.reshape(side, (1,)).astype(jnp.int32), c_blk, c_oth[0])
    return pl.pallas_call(
        append_kernel,
        out_shape=out_shape,
        grid=(2,),
        in_specs=[pl.BlockSpec(memory_space=pl.ANY), pl.BlockSpec((BLK, width), lambda i: (i, 0))],
        out_specs=pl.BlockSpec((BLK, width), lambda i: (i + 6, 0)),
        input_output_aliases={0: 0},
        cost_estimate=cost,
    )(most, c_oth[1])


def butterfly(vec):
    for mask in (1, 2, 4):
        vec = vec + swap(vec, mask)
    return vec


def solution(mesh):
    def body(c_blk, w_blk, h_blk):
        side = lax.axis_index("row")
        col = lax.axis_index("col")
        core, chip = lax.rem(col, 2), lax.div(col, 2)
        half = h_blk.shape[1] // 2
        mine = side * half
        theirs = (1 - side) * half

        def reduce_set_x(num, also):
            view = num.reshape(2, 2, 2, BLK, 1024)
            tot = pick(view, core, 1) + swap(pick(view, 1 - core, 1), 1)
            tot = pick(tot, chip, 1) + swap(pick(tot, 1 - chip, 1), 2)
            tot, also = lax.optimization_barrier((tot, also))
            return tot[0] + swap(tot[1], 4), also

        def reduce_set(num):
            view = num.reshape(2, 2, 2, BLK, 1024)
            got = swap(pick(view, 1 - core, 1), 1)
            tot = pick(view, core, 1) + got
            send = jnp.where(core == 0, pick(tot, 1 - chip, 1), tot[1])
            keep = jnp.where(core == 0, pick(tot, chip, 1), tot[0])
            keep = keep + swap_by_core(send, 2, 4)
            away = jnp.where(core == 0, 1, 1 - chip)
            got = swap_by_core(pick(keep, away, 0), 4, 2)
            return pick(keep, 1 - away, 0) + got

        def gather_set(b0, relay=False):
            pieces = {(0, 0, 0): b0}
            for y, x in ((0, 1), (1, 0), (1, 1)):
                if relay and y and x:
                    pieces[(y, x, 0)] = swap(pieces[(1, 0, 0)], 2)
                else:
                    pieces[(y, x, 0)] = swap(b0, 4 * y + 2 * x)
            for y, x in ((0, 0), (0, 1), (1, 0), (1, 1)):
                pieces[(y, x, 1)] = swap(pieces[(y, x, 0)], 1)
            return assemble(pieces)

        def sums(h_part, w_val):
            w_val = lax.optimization_barrier(tuple(w_val))
            part = jnp.stack([h_part, jnp.sum(w_val[0], axis=0) + jnp.sum(w_val[1], axis=0)])
            tot = butterfly(part)
            return tot[0], tot[1]

        c_oth = []
        for p in range(4):
            sent = lax.dynamic_slice(c_blk, (p * 512, theirs), (512, half))
            c_oth.append(swap(lax.optimization_barrier(sent), 4))
        hb = lax.dynamic_slice_in_dim(h_blk, mine, half, 1).astype(BF16)
        hb_theirs = lax.dynamic_slice_in_dim(h_blk, theirs, half, 1).astype(BF16)
        w_own = w_blk.astype(BF16)
        offset = core * 512 + chip * BLK
        w_state = [lax.dynamic_slice_in_dim(w_blk, s * 1024 + offset, BLK, 0) for s in range(2)]
        w_oth = []
        for s in range(2):
            b0 = w_state[s].astype(BF16)
            p10 = swap(b0, 4)
            p11 = swap(p10, 2)
            pieces = {(0, 0, 0): p10, (0, 1, 0): p11, (0, 0, 1): swap(p10, 1), (0, 1, 1): swap(p11, 1)}
            w_oth.append(assemble(pieces))
        w_sum = jnp.sum(w_blk, axis=0)[None, :]
        w_sum = (w_sum + swap(w_sum, 4))[0]
        h_sum = jnp.sum(h_blk, axis=1)[None, :]
        for mask in (1, 2):
            h_sum = h_sum + swap(h_sum, mask)
        h_sum = h_sum[0]
        q_theirs = quotient(lax.dynamic_slice_in_dim(c_blk, theirs, half, 1), w_own, hb_theirs)
        num_t = dot_nw(q_theirs, hb_theirs)
        q_own = quotient(lax.dynamic_slice_in_dim(c_blk, mine, half, 1), w_own, hb)
        q_own = with_layout_constraint(q_own, Layout((0, 1)))
        num_w = num_t + dot_nw(q_own, hb)
        view = num_w.reshape(2, 2, 2, BLK, 1024)
        tot = pick(view, core, 1) + swap(pick(view, 1 - core, 1), 1)
        num_w = pick(tot, chip, 1) + swap(pick(tot, 1 - chip, 1), 2)
        num_h = dot_nh(w_own, q_own)
        w_state = [lax.optimization_barrier(w_state[s] * num_w[s] / h_sum[None, :]) for s in range(2)]
        w_set = [gather_set(w_state[s].astype(BF16), relay=True) for s in range(2)]
        late, _ = lax.optimization_barrier((mine, w_state[1]))
        h_state = lax.dynamic_slice_in_dim(h_blk, late, half, 1)
        for p in range(4):
            w_part = w_oth[p // 2][(p % 2) * 512:(p % 2) * 512 + 512]
            q_oth = quotient(c_oth[p], w_part, hb)
            num_h = num_h + dot_nh(w_part, q_oth)
        counts = [join_rows(side, c_blk, s * 1024, c_oth[2 * s:2 * s + 2]) for s in range(2)]
        h_state = h_state * num_h / w_sum[:, None]
        hb = h_state.astype(BF16)
        h_part = jnp.sum(h_state, axis=1)

        for _ in range(1, SWEEPS - 1):
            h_sum, w_sum = sums(h_part, w_state)
            q_set, w_next, w_gathered = [], [], []
            for s in range(2):
                q_set.append(quotient(counts[s], w_set[s], hb))
                num_w = reduce_set(dot_nw(q_set[s], hb))
                num_w, h_tot = lax.optimization_barrier((num_w, h_sum))
                w_next.append(lax.optimization_barrier(w_state[s] * num_w / h_tot[None, :]))
                w_gathered.append(gather_set(w_next[s].astype(BF16)))
            num_h = dot_nh(w_set[0], q_set[0]) + dot_nh(w_set[1], q_set[1])
            h_state = h_state * num_h / w_sum[:, None]
            hb = h_state.astype(BF16)
            h_part = jnp.sum(h_state, axis=1)
            w_state = w_next
            w_set = w_gathered

        h_sum, w_sum = sums(h_part, w_state)
        h_out = jnp.zeros(h_blk.shape, F32)
        h_fin, h_got = [], []
        num_w = [None, None]
        spans = tuple(zip(CUTS[:-1], CUTS[1:]))
        for j, (lo, hi) in enumerate(spans):
            at = slice(lo, hi)
            q_set = [quotient(counts[s][:, at], w_set[s], hb[:, at]) for s in range(2)]
            num_h = dot_nh(w_set[0], q_set[0]) + dot_nh(w_set[1], q_set[1])
            h_fin.append(h_state[:, at] * num_h / w_sum[:, None])
            h_got.append(swap(h_fin[j], 4))
            for s in range(2):
                part = dot_nw(q_set[s], hb[:, at])
                num_w[s] = part if num_w[s] is None else num_w[s] + part

        def put(out, val, base, j):
            return lax.dynamic_update_slice_in_dim(out, val, base + spans[j][0], 1)

        tot, h_sum = reduce_set_x(num_w[0], h_sum)
        w_fin = [w_state[0] * tot / h_sum[None, :]]
        for j in range(len(spans)):
            h_out = put(h_out, h_fin[j], mine, j)
        num, h_out = lax.optimization_barrier((num_w[1], h_out))
        for j in range(len(spans) - 2):
            h_out = put(h_out, h_got[j], theirs, j)
        tot, h_out = reduce_set_x(num, h_out)
        w_fin.append(w_state[1] * tot / h_sum[None, :])
        h_out = put(h_out, h_got[-2], theirs, len(spans) - 2)
        w_out = jnp.zeros(w_blk.shape, F32)
        w_fin = jnp.stack(w_fin)
        w_x = swap(w_fin, 2)
        got = [(0, 0, w_fin), (1, 0, w_x), (0, 1, swap(w_fin, 1)), (1, 1, swap(w_x, 1))]
        for x, c, val in got:
            start = jnp.bitwise_xor(core, c) * 512 + jnp.bitwise_xor(chip, x) * BLK
            for s in range(2):
                w_out = lax.dynamic_update_slice_in_dim(w_out, val[s], s * 1024 + start, 0)
        w_out, last = lax.optimization_barrier((w_out, h_got[-1]))
        return w_out, put(h_out, last, theirs, len(spans) - 1)


    return jax.shard_map(
        body,
        mesh=mesh,
        in_specs=(P(("part", "row"), "col"), P(("part", "row"), None), P("part", "col")),
        out_specs=(P(("part", "row"), None), P("part", "col")),
        check_vma=False,
    )
```

```python
import functools

import jax
import jax.numpy as jnp
from jax import lax
from jax.experimental import pallas as pl
from jax.experimental.pallas import tpu as pltpu
from jax.experimental.layout import Layout, with_layout_constraint
from jax.sharding import PartitionSpec as P


SWEEPS = 6
BLK = 256
CUTS = (0, 512, 1536, 2560, 3584, 4096)
AXES = ("row", "col")
F32 = jnp.float32
BF16 = jnp.bfloat16


def swap(val, mask):
    return lax.ppermute(val, AXES, [(i, i ^ mask) for i in range(8)])


def swap_by_core(val, mask0, mask1):
    return lax.ppermute(val, AXES, [(i, i ^ (mask1 if i & 1 else mask0)) for i in range(8)])


def dot_nw(q, h_bf):
    return lax.dot_general(q, h_bf, (((1,), (1,)), ((), ())), preferred_element_type=F32)


def dot_nh(w_bf, q):
    return lax.dot_general(w_bf, q, (((0,), (0,)), ((), ())), preferred_element_type=F32)


def quotient(counts, w_bf, h_bf):
    return (counts.astype(F32) / jnp.dot(w_bf, h_bf, preferred_element_type=F32)).astype(BF16)


def pick(arr, idx, axis):
    return lax.dynamic_index_in_dim(arr, idx, axis, keepdims=False)


def assemble_kernel(keys, axis_col, *refs):
    pieces, out_ref, sems = refs[:len(keys)], refs[-2], refs[-1]
    col = lax.axis_index(axis_col)
    core, chip = lax.rem(col, 2), lax.div(col, 2)
    copies = []
    for n, (yrel, xrel, crel) in enumerate(keys):
        core_at = 1 - core if crel else core
        chip_at = 1 - chip if xrel else chip
        start = pl.multiple_of(yrel * 1024 + core_at * 512 + chip_at * BLK, BLK)
        copy = pltpu.make_async_copy(pieces[n], out_ref.at[pl.ds(start, BLK)], sems.at[n])
        copy.start()
        copies.append(copy)
    for copy in copies:
        copy.wait()


def assemble(pieces):
    keys = tuple(pieces)
    val = next(iter(pieces.values()))
    size = len(keys) * BLK
    return pl.pallas_call(
        functools.partial(assemble_kernel, keys, "col"),
        out_shape=jax.ShapeDtypeStruct((size, val.shape[1]), val.dtype),
        in_specs=[pl.BlockSpec(memory_space=pl.ANY)] * len(keys),
        out_specs=pl.BlockSpec(memory_space=pltpu.VMEM),
        scratch_shapes=[pltpu.SemaphoreType.DMA((len(keys),))],
        cost_estimate=pl.CostEstimate(flops=10 ** 9, bytes_accessed=4 * size * val.shape[1], transcendentals=0),
    )(*[pieces[k] for k in keys])


def join_kernel(side_ref, own_ref, oth_ref, out_ref):
    step = pl.program_id(0)

    @pl.when(step < 4)
    def _():
        out_ref[...] = own_ref[...]

    @pl.when(step >= 4)
    def _():
        out_ref[...] = oth_ref[...]


def append_kernel(all_ref, oth_ref, out_ref):
    out_ref[...] = oth_ref[...]


def join_rows(side, c_blk, first_row, c_oth):
    width = c_oth[0].shape[1]
    base = first_row // BLK
    out_shape = jax.ShapeDtypeStruct((2048, width), BF16)
    cost = pl.CostEstimate(flops=10 ** 9, bytes_accessed=4 * 1024 * width, transcendentals=0)
    most = pl.pallas_call(
        join_kernel,
        out_shape=out_shape,
        grid_spec=pltpu.PrefetchScalarGridSpec(
            num_scalar_prefetch=1,
            grid=(6,),
            in_specs=[
                pl.BlockSpec((BLK, width), lambda i, s: (base + jnp.minimum(i, 3), s[0])),
                pl.BlockSpec((BLK, width), lambda i, s: (jnp.maximum(i - 4, 0), 0)),
            ],
            out_specs=pl.BlockSpec((BLK, width), lambda i, s: (i, 0)),
        ),
        cost_estimate=cost,
    )(jnp.reshape(side, (1,)).astype(jnp.int32), c_blk, c_oth[0])
    return pl.pallas_call(
        append_kernel,
        out_shape=out_shape,
        grid=(2,),
        in_specs=[pl.BlockSpec(memory_space=pl.ANY), pl.BlockSpec((BLK, width), lambda i: (i, 0))],
        out_specs=pl.BlockSpec((BLK, width), lambda i: (i + 6, 0)),
        input_output_aliases={0: 0},
        cost_estimate=cost,
    )(most, c_oth[1])


def butterfly(vec):
    for mask in (1, 2, 4):
        vec = vec + swap(vec, mask)
    return vec


def solution(mesh):
    def body(c_blk, w_blk, h_blk):
        side = lax.axis_index("row")
        col = lax.axis_index("col")
        core, chip = lax.rem(col, 2), lax.div(col, 2)
        half = h_blk.shape[1] // 2
        mine = side * half
        theirs = (1 - side) * half

        def reduce_set_x(num, also):
            view = num.reshape(2, 2, 2, BLK, 1024)
            tot = pick(view, core, 1) + swap(pick(view, 1 - core, 1), 1)
            tot = pick(tot, chip, 1) + swap(pick(tot, 1 - chip, 1), 2)
            tot, also = lax.optimization_barrier((tot, also))
            return tot[0] + swap(tot[1], 4), also

        def reduce_set(num):
            view = num.reshape(2, 2, 2, BLK, 1024)
            got = swap(pick(view, 1 - core, 1), 1)
            tot = pick(view, core, 1) + got
            send = jnp.where(core == 0, pick(tot, 1 - chip, 1), tot[1])
            keep = jnp.where(core == 0, pick(tot, chip, 1), tot[0])
            keep = keep + swap_by_core(send, 2, 4)
            away = jnp.where(core == 0, 1, 1 - chip)
            got = swap_by_core(pick(keep, away, 0), 4, 2)
            return pick(keep, 1 - away, 0) + got

        def gather_set(b0, relay=False):
            pieces = {(0, 0, 0): b0}
            for y, x in ((0, 1), (1, 0), (1, 1)):
                if relay and y and x:
                    pieces[(y, x, 0)] = swap(pieces[(1, 0, 0)], 2)
                else:
                    pieces[(y, x, 0)] = swap(b0, 4 * y + 2 * x)
            for y, x in ((0, 0), (0, 1), (1, 0), (1, 1)):
                pieces[(y, x, 1)] = swap(pieces[(y, x, 0)], 1)
            return assemble(pieces)

        def sums(h_part, w_val):
            w_val = lax.optimization_barrier(tuple(w_val))
            part = jnp.stack([h_part, jnp.sum(w_val[0], axis=0) + jnp.sum(w_val[1], axis=0)])
            tot = butterfly(part)
            return tot[0], tot[1]

        c_oth = []
        for p in range(4):
            sent = lax.dynamic_slice(c_blk, (p * 512, theirs), (512, half))
            c_oth.append(swap(lax.optimization_barrier(sent), 4))
        hb = lax.dynamic_slice_in_dim(h_blk, mine, half, 1).astype(BF16)
        hb_theirs = lax.dynamic_slice_in_dim(h_blk, theirs, half, 1).astype(BF16)
        w_own = w_blk.astype(BF16)
        offset = core * 512 + chip * BLK
        w_state = [lax.dynamic_slice_in_dim(w_blk, s * 1024 + offset, BLK, 0) for s in range(2)]
        w_oth = []
        for s in range(2):
            b0 = w_state[s].astype(BF16)
            p10 = swap(b0, 4)
            p11 = swap(p10, 2)
            pieces = {(0, 0, 0): p10, (0, 1, 0): p11, (0, 0, 1): swap(p10, 1), (0, 1, 1): swap(p11, 1)}
            w_oth.append(assemble(pieces))
        w_sum = jnp.sum(w_blk, axis=0)[None, :]
        w_sum = (w_sum + swap(w_sum, 4))[0]
        h_sum = jnp.sum(h_blk, axis=1)[None, :]
        for mask in (1, 2):
            h_sum = h_sum + swap(h_sum, mask)
        h_sum = h_sum[0]
        q_theirs = quotient(lax.dynamic_slice_in_dim(c_blk, theirs, half, 1), w_own, hb_theirs)
        num_t = dot_nw(q_theirs, hb_theirs)
        q_own = quotient(lax.dynamic_slice_in_dim(c_blk, mine, half, 1), w_own, hb)
        q_own = with_layout_constraint(q_own, Layout((0, 1)))
        num_w = num_t + dot_nw(q_own, hb)
        view = num_w.reshape(2, 2, 2, BLK, 1024)
        tot = pick(view, core, 1) + swap(pick(view, 1 - core, 1), 1)
        num_w = pick(tot, chip, 1) + swap(pick(tot, 1 - chip, 1), 2)
        num_h = dot_nh(w_own, q_own)
        w_state = [lax.optimization_barrier(w_state[s] * num_w[s] / h_sum[None, :]) for s in range(2)]
        w_set = [gather_set(w_state[s].astype(BF16), relay=True) for s in range(2)]
        late, _ = lax.optimization_barrier((mine, w_state[1]))
        h_state = lax.dynamic_slice_in_dim(h_blk, late, half, 1)
        for p in range(4):
            w_part = w_oth[p // 2][(p % 2) * 512:(p % 2) * 512 + 512]
            q_oth = quotient(c_oth[p], w_part, hb)
            num_h = num_h + dot_nh(w_part, q_oth)
        counts = [join_rows(side, c_blk, s * 1024, c_oth[2 * s:2 * s + 2]) for s in range(2)]
        h_state = h_state * num_h / w_sum[:, None]
        hb = h_state.astype(BF16)
        h_part = jnp.sum(h_state, axis=1)

        for _ in range(1, SWEEPS - 1):
            h_sum, w_sum = sums(h_part, w_state)
            q_set, w_next, w_gathered = [], [], []
            for s in range(2):
                q_set.append(quotient(counts[s], w_set[s], hb))
                num_w = reduce_set(dot_nw(q_set[s], hb))
                num_w, h_tot = lax.optimization_barrier((num_w, h_sum))
                w_next.append(lax.optimization_barrier(w_state[s] * num_w / h_tot[None, :]))
                w_gathered.append(gather_set(w_next[s].astype(BF16)))
            num_h = dot_nh(w_set[0], q_set[0]) + dot_nh(w_set[1], q_set[1])
            h_state = h_state * num_h / w_sum[:, None]
            hb = h_state.astype(BF16)
            h_part = jnp.sum(h_state, axis=1)
            w_state = w_next
            w_set = w_gathered

        h_sum, w_sum = sums(h_part, w_state)
        h_out = jnp.zeros(h_blk.shape, F32)
        h_fin, h_got = [], []
        num_w = [None, None]
        spans = tuple(zip(CUTS[:-1], CUTS[1:]))
        for j, (lo, hi) in enumerate(spans):
            at = slice(lo, hi)
            q_set = [quotient(counts[s][:, at], w_set[s], hb[:, at]) for s in range(2)]
            num_h = dot_nh(w_set[0], q_set[0]) + dot_nh(w_set[1], q_set[1])
            h_fin.append(h_state[:, at] * num_h / w_sum[:, None])
            h_got.append(swap(h_fin[j], 4))
            for s in range(2):
                part = dot_nw(q_set[s], hb[:, at])
                num_w[s] = part if num_w[s] is None else num_w[s] + part

        def put(out, val, base, j):
            return lax.dynamic_update_slice_in_dim(out, val, base + spans[j][0], 1)

        tot, h_sum = reduce_set_x(num_w[0], h_sum)
        w_fin = [w_state[0] * tot / h_sum[None, :]]
        for j in range(len(spans)):
            h_out = put(h_out, h_fin[j], mine, j)
        num, h_out = lax.optimization_barrier((num_w[1], h_out))
        for j in range(len(spans) - 2):
            h_out = put(h_out, h_got[j], theirs, j)
        tot, h_out = reduce_set_x(num, h_out)
        w_fin.append(w_state[1] * tot / h_sum[None, :])
        h_out = put(h_out, h_got[-2], theirs, len(spans) - 2)
        w_out = jnp.zeros(w_blk.shape, F32)
        for s in range(2):
            w_x = swap(w_fin[s], 2)
            got = [(0, 0, w_fin[s]), (1, 0, w_x), (0, 1, swap(w_fin[s], 1)), (1, 1, swap(w_x, 1))]
            for x, c, val in got:
                at = s * 1024 + jnp.bitwise_xor(core, c) * 512 + jnp.bitwise_xor(chip, x) * BLK
                w_out = lax.dynamic_update_slice_in_dim(w_out, val, at, 0)
        w_out, last = lax.optimization_barrier((w_out, h_got[-1]))
        return w_out, put(h_out, last, theirs, len(spans) - 1)


    return jax.shard_map(
        body,
        mesh=mesh,
        in_specs=(P(("part", "row"), "col"), P(("part", "row"), None), P("part", "col")),
        out_specs=(P(("part", "row"), None), P("part", "col")),
        check_vma=False,
    )
```
